256 devices in a mesh: section: 4 (over y_lo, core), expert: 64 (over y_hi, x, z).
Axes of the slice: x: 4, y: 4 (y_hi: 2, y_lo: 2; y = y_hi * 2 + y_lo), z: 8, core: 2. Of those that a mesh axis runs over, the one named last changes fastest.
Arguments:
- activations: bfloat16 [4, 2048, 4096], P('section', 'expert'), may hold values from -6 to 6
- norm_gain: float32 [4, 4096], P('section'), may hold values from 0.25 to 1.75
- in_proj: bfloat16 [4, 4096, 40960], P('section', None, 'expert'), may hold values from -0.09375 to 0.09375
- out_proj: bfloat16 [4, 40960, 4096], P('section', 'expert'), may hold values from -0.078125 to 0.078125
- expert_ids: int32 [4, 2048, 1], P('section', 'expert'), may hold values from 0 to 7; in each aligned block of 32 rows (0 to 31, 32 to 63, ..., all dimensions but the last counted through in order) at most 8 rows name the same one
Outputs:
- passed: bfloat16 [4, 2048, 4096], P('section', 'expert')
The draws below stay inside these ranges and needn't reach their ends.
Inputs may be any that keep to these rules, and one draw needn't show every extreme that they name: `expert_ids`: within the 32 rows of one device (aligned blocks of 32 rows along the token dimension of each layer), no expert is named by more than 8 rows.
All inputs are finite; a program needn't handle non-finite values.
Results may differ from the reference program's by a relative error of at most 0.0047.
Values may be sent and summed in bfloat16 or wider, within the bound.
A program may use at most 64 MiB of HBM per device.

```python
import math
import jax
import jax.numpy as jnp
import numpy as np
from jax import lax

D = 4096
FF_W = 5120
EXPERTS = 8
MB_TOK = 32
CAP = 8
TOKENS = 2048
N_SECTION = 4
N_EXPERT = 64


def steps_of(stream_key, dims, split, smallest, largest):
    gain, own = 1.0, jax.random.fold_in(stream_key, 6)
    for dim, parts in split:
        steps = jnp.exp(jax.random.uniform(jax.random.fold_in(own, dim), (parts,), jnp.float32, smallest / len(split), largest / len(split)))
        gain = gain * jnp.repeat(steps, dims[dim] // parts).reshape([-1 if axis == dim else 1 for axis in range(len(dims))])
    return gain


def shared_out(own_key, own, number, rows, number_of, top, bound, lean):
    order = jax.random.permutation(own_key, number_of)
    heavy_load, common = portions_of(number_of, rows * top, bound, lean, True), portions_of(number_of, rows * top, bound, lean, False)
    places = jnp.arange(number_of)

    def named(lengths, turn):
        used = int((lengths > 0).sum())
        fixed = max(1, used // 4)
        shifted = fixed + (places - fixed + turn * (used - fixed)) % max(1, number_of - fixed)
        return jnp.zeros((number_of,), jnp.int32).at[order[jnp.where(places < fixed, places, shifted)]].set(jnp.asarray(lengths, jnp.int32))

    lengths = jnp.where(number % 4 == 0, named(heavy_load, number // 4), named(common, number - number // 4 - 1))
    mixed = jax.random.permutation(jax.random.fold_in(own, 3), number_of)
    source_of, sink = mixed[0:number_of // 2 * 2:2], mixed[1:number_of // 2 * 2:2]
    margin = jnp.minimum(lengths[source_of] - 1, bound - lengths[sink]) // 2
    margin = jnp.where((source_of == order[0]) | (sink == order[0]) | (lengths[sink] == 0), 0, jnp.maximum(margin, 0))
    shifted = jax.random.randint(jax.random.fold_in(own, 4), (number_of // 2,), 0, 1 << 20) % (margin + 1)
    lengths = lengths.at[source_of].add(-shifted).at[sink].add(shifted)
    members = jnp.searchsorted(jnp.cumsum(lengths), jnp.arange(rows * top), side="right").astype(jnp.int32)
    listing = members.reshape(top, rows).T
    listing = listing[jax.random.permutation(jax.random.fold_in(own, 1), rows)]
    turn = jax.random.randint(jax.random.fold_in(own, 2), (rows, 1), 0, top)
    return jnp.take_along_axis(listing, (jnp.arange(top)[None, :] + turn) % top, axis=1)


def portions_of(count, total, most, slope, full):
    portions = [(1 << 20) // math.isqrt(grade ** slope) + 1 for grade in range(1, count + 1)]
    largest = most if full else min(most, max(-(-total // count), total * portions[0] // sum(portions)))
    least = 1 if total - largest >= count - 1 else 0
    given, spare = [largest] + [least] * (count - 1), total - largest - least * (count - 1)
    while spare > 0:
        candidates = [i for i in range(1, count) if given[i] < largest] or [i for i in range(1, count) if given[i] < most]
        mass, remaining = sum([portions[i] for i in candidates]), spare
        for i in candidates:
            extra = min(most - given[i], max(1, remaining * portions[i] // mass), spare)
            given[i] = given[i] + extra
            spare = spare - extra
    return np.array(given)


def centred(key, shape, width, most, shards=(), kind=jnp.bfloat16):
    factor_of = steps_of(key, shape, shards, -0.22, 0.18) if shards else 1.0
    drawn = jax.random.normal(key, shape, jnp.float32) * width * factor_of
    return jnp.minimum(jnp.maximum(drawn, -most), most).astype(kind)


def setup_inputs(seed: int = 0) -> dict:
    key_list = jax.random.split(jax.random.key(seed), 6)
    activations = centred(key_list[0], (N_SECTION, TOKENS, D), 1.0, 6.0, ((0, 4), (1, 64)))
    norm_gain = jnp.clip(1.0 + 0.15 * jax.random.normal(key_list[1], (N_SECTION, D), jnp.float32), 0.25, 1.75)
    in_proj = centred(key_list[2], (N_SECTION, D, EXPERTS * FF_W), D ** -0.5, 0.09375, ((0, 4), (2, 64)))
    out_proj = centred(key_list[3], (N_SECTION, EXPERTS * FF_W, D), FF_W ** -0.5, 0.078125, ((0, 4), (1, 64)))
    expert_ids_keys = jax.random.split(jax.random.fold_in(key_list[4], 1), N_SECTION * TOKENS // MB_TOK)
    expert_ids_turns = jax.random.permutation(jax.random.fold_in(key_list[4], 3), N_SECTION * TOKENS // MB_TOK)
    expert_ids = jax.vmap(lambda own, number: shared_out(jax.random.fold_in(key_list[4], 2), own, number, MB_TOK, EXPERTS, 1, CAP, 2))(expert_ids_keys, expert_ids_turns).reshape((N_SECTION, TOKENS, 1))
    return {"activations": activations, "norm_gain": norm_gain, "in_proj": in_proj, "out_proj": out_proj, "expert_ids": expert_ids}


epsilon = 1e-06

def reference(activations, norm_gain, in_proj, out_proj, expert_ids):
    groups = N_EXPERT // EXPERTS
    slice_width = FF_W // groups
    results = []
    for section_index in range(N_SECTION):
        floats = activations[section_index].astype(jnp.float32)
        scale = lax.rsqrt(lax.optimization_barrier(jnp.mean(floats * floats, axis=-1, keepdims=True)) + epsilon)
        normed = (floats * scale * norm_gain[section_index][None, :]).astype(jnp.bfloat16)
        routed = expert_ids[section_index, :, 0].astype(jnp.int32)
        onehot = (routed[:, None] == jnp.arange(EXPERTS, dtype=jnp.int32)[None, :]).astype(jnp.int32)
        blocked = onehot.reshape(N_EXPERT, MB_TOK, EXPERTS)
        before = (jnp.cumsum(blocked, axis=1) - blocked).reshape(TOKENS, EXPERTS)
        ranks = lax.optimization_barrier(jnp.sum(before * onehot, axis=1)).astype(jnp.int32)
        slots = (jnp.arange(TOKENS, dtype=jnp.int32) // MB_TOK * CAP + ranks).astype(jnp.int32)
        buffer = jnp.zeros((EXPERTS, N_EXPERT * CAP, D), jnp.bfloat16).at[routed, slots].set(normed)
        first_proj = in_proj[section_index].reshape(D, EXPERTS, FF_W).transpose(1, 0, 2)
        second_proj = out_proj[section_index].reshape(EXPERTS, FF_W, D)

        def expert(operands):
            inputs, first, second = operands
            preact = jnp.dot(inputs, first, preferred_element_type=jnp.float32)
            hidden = jax.nn.gelu(preact, approximate=True).astype(jnp.bfloat16)
            summed = jnp.zeros((inputs.shape[0], D), jnp.float32)
            for shard in range(groups):
                piece = jnp.dot(hidden[:, shard * slice_width:(shard + 1) * slice_width], second[shard * slice_width:(shard + 1) * slice_width], preferred_element_type=jnp.float32)
                summed = summed + piece
            return summed
        outputs = lax.map(expert, (buffer, first_proj, second_proj))
        mixed_rows = outputs[routed, slots]
        results.append((floats + mixed_rows).astype(jnp.bfloat16))
    return jnp.roll(jnp.stack(results), 1, axis=0)
```

```python
import functools

import jax
import jax.numpy as jnp
from jax import lax
from jax.experimental import pallas as pl
from jax.experimental.pallas import tpu as pltpu
from jax.sharding import PartitionSpec as P

MESH = pl.DeviceIdType.MESH
EPS = 1e-06
NZ = 8
NR = 8
NX = 4
CAP = 8
ROWS = NR * CAP
CA = 2048
CHUNK = 1024

ZI = {0: 0, 1: 1, -1: 2, 2: 3, -2: 4, 3: 5, -3: 6, 4: 7, -4: 7}
FAR = {(1, 0): 4, (1, 1): 3, (-1, 0): 3, (-1, 1): 4}
CHAINS = [(1, 0), (1, 1), (-1, 0), (-1, 1)]


def opposite(r):
    return r // NX * NX + (NX - r % NX) % NX


def kernel(
    act, gain, ids, w1_hbm, w2_hbm, out,
    w1, w2, codes, gathered, packed_a, packed_b, xa, xb, pre, own_a, back_b,
    ret_b, own_b, sum_a, ret_a, final,
    send_a, land_a, send_b, land_b,
    w_sem, one_send, one_recv, ag_recv, plane_recv, rs_recv,
):
    tokens, width = act.shape
    cb = width - CA
    s = lax.axis_index("section")
    e = lax.axis_index("expert")
    z, p = lax.rem(e, NZ), e // NZ
    yh, x = p // NX, lax.rem(p, NX)

    def z_dev(k):
        return (s, p * NZ + lax.rem(z + k + NZ, NZ))

    def plane_of(r):
        return lax.rem(yh + r // NX, NR // NX) * NX + lax.rem(x + r % NX, NX)

    def r_dev(r):
        return (s, plane_of(r) * NZ + z)

    sections = lax.axis_size("section")
    ahead = (lax.rem(s + 1, sections), e)
    behind = (lax.rem(s + sections - 1, sections), e)

    def remote(src, dst, send, recv, to):
        return pltpu.make_async_remote_copy(
            src_ref=src, dst_ref=dst, send_sem=send, recv_sem=recv,
            device_id=to, device_id_type=MESH,
        )

    def drain(ref, sem):
        pltpu.make_async_copy(ref, ref, sem).wait()

    load_w1 = pltpu.make_async_copy(w1_hbm, w1, w_sem.at[0])
    load_w2 = pltpu.make_async_copy(w2_hbm, w2, w_sem.at[1])
    load_w1.start()
    load_w2.start()

    barrier = pltpu.get_barrier_semaphore()
    peers = [r_dev(r) for r in range(1, NR)] + [z_dev(k) for k in range(1, NZ)]
    for to in peers + [ahead, behind]:
        pl.semaphore_signal(barrier, inc=1, device_id=to, device_id_type=MESH)

    floats = act[...].astype(jnp.float32)
    scale = lax.rsqrt(jnp.mean(floats * floats, axis=-1, keepdims=True) + EPS)
    normed = (floats * scale * gain[...]).astype(jnp.bfloat16)
    gathered[0] = normed[:, CA:]

    col = jnp.broadcast_to(ids[...], (tokens, 128))[:, :tokens]
    i0 = lax.broadcasted_iota(jnp.int32, (tokens, tokens), 0)
    i1 = lax.broadcasted_iota(jnp.int32, (tokens, tokens), 1)
    row = jnp.sum(jnp.where(i0 == i1, col, 0), axis=0, keepdims=True)
    rank = jnp.sum(
        jnp.where((col == row) & (i0 < i1), 1, 0), axis=0, keepdims=True
    )
    code = row * CAP + rank
    codes[0, :, 0:tokens] = jnp.broadcast_to(code, (8, tokens))

    slot = lax.broadcasted_iota(jnp.int32, (ROWS, tokens), 0)
    rel = slot // CAP
    expert_of = lax.rem(yh + rel // NX, NR // NX) * NX + lax.rem(x + lax.rem(rel, NX), NX)
    wanted = expert_of * CAP + lax.rem(slot, CAP)

    def placing(i):
        return jnp.where(wanted == codes[i, 0:1, 0:tokens], 1.0, 0.0).astype(jnp.bfloat16)

    def pack(place, rows):
        return jnp.dot(place, rows, preferred_element_type=jnp.float32).astype(jnp.bfloat16)

    def unpack(place, slots):
        return lax.dot_general(
            place, slots, (((0,), (0,)), ((), ())), preferred_element_type=jnp.float32
        )

    place_own = jnp.where(wanted == code, 1.0, 0.0).astype(jnp.bfloat16)
    packed_a[...] = pack(place_own, normed[:, :CA]).reshape(NR, CAP, CA)

    pl.semaphore_wait(barrier, len(peers) + 2)

    def ag_copy(buf, kind, d, h, k, cols):
        half = cols // 2
        at = pl.ds(h * half, half)
        if kind == 0:
            src, dst = buf.at[ZI[d * k], :, :, at], buf.at[ZI[d * (k + 1)], :, :, at]
        else:
            src, dst = buf.at[ZI[d * k], :, at], buf.at[ZI[d * (k + 1)], :, at]
        chain = CHAINS.index((d, h))
        return remote(
            src, dst, one_send.at[kind], ag_recv.at[kind, chain, k], z_dev(d)
        )

    def ag_a(d, h, k):
        return ag_copy(xa, 0, d, h, k, CA)

    def ag_b(d, h, k):
        return ag_copy(gathered, 1, d, h, k, cb)

    def forward(ag, k):
        for d, h in CHAINS:
            if k <= FAR[d, h]:
                ag(d, h, k - 1).wait_recv()
                if k < FAR[d, h]:
                    ag(d, h, k).start()

    for d, h in CHAINS:
        ag_b(d, h, 0).start()
    for k in range(1, NZ):
        remote(codes.at[0], codes.at[NZ - k], one_send.at[2], one_recv.at[0], z_dev(k)).start()

    for r in range(1, NR):
        remote(
            packed_a.at[r], xa.at[0, opposite(r)], one_send.at[3], one_recv.at[1], r_dev(r)
        ).start()
    xa[0, 0] = packed_a[0]

    def send_packed(i, place):
        packed_b[i] = pack(place, gathered[i]).reshape(NR, CAP, cb)
        for r in range(1, NR):
            remote(
                packed_b.at[i, r], xb.at[i, opposite(r)],
                one_send.at[4], plane_recv.at[0, i], r_dev(r),
            ).start()
        xb[i, 0] = packed_b[i, 0]

    send_packed(0, place_own)
    drain(xa.at[0, pl.ds(1, NR - 1)], one_recv.at[1])
    for d, h in CHAINS:
        ag_a(d, h, 0).start()
    forward(ag_b, 1)
    drain(codes.at[pl.ds(1, NZ - 1)], one_recv.at[0])

    def place_of(i):
        k = [d for d in range(-3, 5) if ZI[d] == i][0]
        return placing((-k) % NZ)

    for i in (1, 2):
        send_packed(i, place_of(i))
    forward(ag_b, 2)
    for i in (3, 4):
        send_packed(i, place_of(i))
    forward(ag_a, 1)
    load_w1.wait()
    load_w2.wait()

    def ffn(i, n):
        rows = n * ROWS
        for c in range(0, width, CHUNK):
            if c < CA:
                block = xa[i:i + n, :, :, c:c + CHUNK]
            else:
                block = xb[i:i + n, :, :, c - CA:c - CA + CHUNK]
            term = jnp.dot(
                block.reshape(rows, CHUNK), w1[c:c + CHUNK, :],
                preferred_element_type=jnp.float32,
            )
            if c == 0:
                pre[0:rows, :] = term
            else:
                pre[0:rows, :] += term
        hidden = jax.nn.gelu(pre[0:rows, :], approximate=True).astype(jnp.bfloat16)
        for c in range(0, width, CHUNK):
            part = jnp.dot(
                hidden, w2[:, c:c + CHUNK], preferred_element_type=jnp.float32
            )
            if c < CA:
                own_a[i:i + n, :, c:c + CHUNK] = part.reshape(n, ROWS, CHUNK)
            else:
                back_b[i:i + n, :, :, c - CA:c - CA + CHUNK] = (
                    part.astype(jnp.bfloat16).reshape(n, NR, CAP, CHUNK)
                )

    def run(i, n):
        for j in range(i, i + n):
            drain(xb.at[j, pl.ds(1, NR - 1)], plane_recv.at[0, j])
        ffn(i, n)
        for j in range(i, i + n):
            for r in range(1, NR):
                remote(
                    back_b.at[j, r], ret_b.at[j, opposite(r)],
                    one_send.at[5], plane_recv.at[1, j], r_dev(r),
                ).start()
            ret_b[j, 0] = back_b[j, 0]

    run(0, 1)
    forward(ag_b, 3)
    for i in (5, 6):
        send_packed(i, place_of(i))
    forward(ag_a, 2)
    run(1, 2)
    forward(ag_b, 4)
    send_packed(7, place_of(7))
    forward(ag_a, 3)
    run(3, 2)
    forward(ag_a, 4)

    def rs_copy(kind, d, h, k):
        send, land = ((send_a, land_a), (send_b, land_b))[kind]
        chain = CHAINS.index((d, h))
        return remote(
            send.at[chain, k - 1], land.at[chain, k - 1],
            one_send.at[6 + kind], rs_recv.at[kind, chain, k - 1], z_dev(-d),
        )

    def rs_own(kind, d, h, k):
        own, cols = ((own_a, CA), (own_b, cb))[kind]
        half = cols // 2
        return own[ZI[d * k], :, h * half:(h + 1) * half]

    def rs_head(kind, k):
        for d, h in CHAINS:
            if k == FAR[d, h]:
                send = (send_a, send_b)[kind]
                send[CHAINS.index((d, h)), k - 1] = rs_own(kind, d, h, k).astype(jnp.bfloat16)
                rs_copy(kind, d, h, k).start()

    def rs_step(kind, k):
        send, land = ((send_a, land_a), (send_b, land_b))[kind]
        for d, h in CHAINS:
            if k < FAR[d, h]:
                chain = CHAINS.index((d, h))
                rs_copy(kind, d, h, k + 1).wait_recv()
                send[chain, k - 1] = (
                    rs_own(kind, d, h, k) + land[chain, k].astype(jnp.float32)
                ).astype(jnp.bfloat16)
                rs_copy(kind, d, h, k).start()

    def rs_last(kind, h):
        land = (land_a, land_b)[kind]
        total = rs_own(kind, 1, h, 0)
        for d in (1, -1):
            rs_copy(kind, d, h, 1).wait_recv()
            total = total + land[CHAINS.index((d, h)), 0].astype(jnp.float32)
        return total

    def take_b(i):
        drain(ret_b.at[i, pl.ds(1, NR - 1)], plane_recv.at[1, i])
        own_b[i] = unpack(place_of(i), ret_b[i].reshape(ROWS, cb))

    run(5, 2)
    rs_head(0, 3)
    run(7, 1)
    rs_head(0, 4)
    rs_step(0, 3)
    rs_step(0, 2)
    for i in (5, 6):
        take_b(i)
    rs_head(1, 3)
    take_b(7)
    rs_head(1, 4)
    rs_step(0, 1)
    for i in (3, 4):
        take_b(i)
    rs_step(1, 3)
    half = CA // 2
    for h in range(2):
        sum_a[:, :, h * half:(h + 1) * half] = (
            rs_last(0, h).astype(jnp.bfloat16).reshape(NR, CAP, half)
        )
    for r in range(1, NR):
        remote(
            sum_a.at[r], ret_a.at[opposite(r)], one_send.at[8], one_recv.at[2], r_dev(r)
        ).start()
    ret_a[0] = sum_a[0]
    rs_step(1, 2)
    for i in (1, 2):
        take_b(i)
    rs_step(1, 1)
    take_b(0)

    drain(ret_a.at[pl.ds(1, NR - 1)], one_recv.at[2])
    final[:, :CA] = (
        act[:, :CA].astype(jnp.float32) + unpack(place_own, ret_a[...].reshape(ROWS, CA))
    ).astype(jnp.bfloat16)
    out_a = remote(
        final.at[:, pl.ds(0, CA)], out.at[:, pl.ds(0, CA)], one_send.at[9], one_recv.at[3], ahead
    )
    out_a.start()
    half = cb // 2
    for h in range(2):
        at = slice(CA + h * half, CA + (h + 1) * half)
        final[:, at] = (act[:, at].astype(jnp.float32) + rs_last(1, h)).astype(jnp.bfloat16)
    out_b = remote(
        final.at[:, pl.ds(CA, cb)], out.at[:, pl.ds(CA, cb)], one_send.at[10], one_recv.at[4], ahead
    )
    out_b.start()

    drain(xa.at[pl.ds(1, NZ - 1)], one_send.at[0])
    drain(gathered.at[pl.ds(1, NZ - 1)], one_send.at[1])
    drain(codes.at[pl.ds(1, NZ - 1)], one_send.at[2])
    drain(packed_a.at[pl.ds(1, NR - 1)], one_send.at[3])
    drain(packed_b.at[:, pl.ds(1, NR - 1)], one_send.at[4])
    drain(back_b.at[:, pl.ds(1, NR - 1)], one_send.at[5])
    drain(xa.at[pl.ds(1, NZ - 1)], one_send.at[6])
    drain(gathered.at[pl.ds(1, NZ - 1)], one_send.at[7])
    drain(sum_a.at[pl.ds(1, NR - 1)], one_send.at[8])
    out_a.wait()
    out_b.wait()


def per_device(activations, norm_gain, in_proj, out_proj, expert_ids):
    _, tokens, width = activations.shape
    hidden = in_proj.shape[2]
    cb = width - CA
    bf16, f32 = jnp.bfloat16, jnp.float32
    vmem = pl.BlockSpec(memory_space=pltpu.VMEM)
    hbm = pl.BlockSpec(memory_space=pl.ANY)
    out = pl.pallas_call(
        kernel,
        out_shape=jax.ShapeDtypeStruct((tokens, width), bf16),
        in_specs=[vmem, vmem, vmem, hbm, hbm],
        out_specs=vmem,
        scratch_shapes=[
            pltpu.VMEM((width, hidden), bf16),
            pltpu.VMEM((hidden, width), bf16),
            pltpu.VMEM((NZ, 8, 128), jnp.int32),
            pltpu.VMEM((NZ, tokens, cb), bf16),
            pltpu.VMEM((NR, CAP, CA), bf16),
            pltpu.VMEM((NZ, NR, CAP, cb), bf16),
            pltpu.VMEM((NZ, NR, CAP, CA), bf16),
            pltpu.VMEM((NZ, NR, CAP, cb), bf16),
            pltpu.VMEM((2 * ROWS, hidden), f32),
            pltpu.VMEM((NZ, ROWS, CA), f32),
            pltpu.VMEM((NZ, NR, CAP, cb), bf16),
            pltpu.VMEM((NZ, NR, CAP, cb), bf16),
            pltpu.VMEM((NZ, tokens, cb), f32),
            pltpu.VMEM((NR, CAP, CA), bf16),
            pltpu.VMEM((NR, CAP, CA), bf16),
            pltpu.VMEM((tokens, width), bf16),
            pltpu.VMEM((4, 4, ROWS, CA // 2), bf16),
            pltpu.VMEM((4, 4, ROWS, CA // 2), bf16),
            pltpu.VMEM((4, 4, tokens, cb // 2), bf16),
            pltpu.VMEM((4, 4, tokens, cb // 2), bf16),
            pltpu.SemaphoreType.DMA((2,)),
            pltpu.SemaphoreType.DMA((11,)),
            pltpu.SemaphoreType.DMA((5,)),
            pltpu.SemaphoreType.DMA((2, 4, 4)),
            pltpu.SemaphoreType.DMA((2, NZ)),
            pltpu.SemaphoreType.DMA((2, 4, 4)),
        ],
        compiler_params=pltpu.CompilerParams(
            collective_id=0, has_side_effects=True, vmem_limit_bytes=58 * 2**20
        ),
    )(activations[0], norm_gain, expert_ids[0], in_proj[0], out_proj[0])
    return out[None]


def solution(mesh):
    return jax.shard_map(
        per_device,
        mesh=mesh,
        in_specs=(
            P("section", "expert", None),
            P("section", None),
            P("section", None, "expert"),
            P("section", "expert", None),
            P("section", "expert", None),
        ),
        out_specs=P("section", "expert", None),
        check_vma=False,
    )
```

```python
import functools

import jax
import jax.numpy as jnp
from jax import lax
from jax.experimental import pallas as pl
from jax.experimental.pallas import tpu as pltpu
from jax.sharding import PartitionSpec as P

MESH = pl.DeviceIdType.MESH
EPS = 1e-06
NZ = 8
NR = 8
NX = 4
CAP = 8
GROUPS = 2
PART = NR // GROUPS
ROWS = NR * CAP
CA = 2048
CHUNK = 1024

ZI = {0: 0, 1: 1, -1: 2, 2: 3, -2: 4, 3: 5, -3: 6, 4: 7, -4: 7}
FAR = {(1, 0): 4, (1, 1): 3, (-1, 0): 3, (-1, 1): 4}
CHAINS = [(1, 0), (-1, 1), (1, 1), (-1, 0)]


def opposite(r):
    return r // NX * NX + (NX - r % NX) % NX


def kernel(
    act_hbm, gain_hbm, ids_hbm, w1_hbm, w2_hbm, out,
    act, gain, ids, before, w1, w2, codes, gathered, packed_a, packed_b, xa, xb, pre, own_a, back_b,
    ret_b, own_b, sum_a, ret_a, tail_b,
    send_a, land_a, send_b, land_b,
    w_sem, one_send, one_recv, ag_recv, plane_recv, rs_recv,
):
    tokens, width = act_hbm.shape
    cb = width - CA
    s = lax.axis_index("section")
    e = lax.axis_index("expert")
    z, p = lax.rem(e, NZ), e // NZ
    yh, x = p // NX, lax.rem(p, NX)

    def z_dev(k, section=s):
        return (section, p * NZ + lax.rem(z + k + NZ, NZ))

    def plane_of(r):
        return lax.rem(yh + r // NX, NR // NX) * NX + lax.rem(x + r % NX, NX)

    def r_dev(r, section=s):
        return (section, plane_of(r) * NZ + z)

    sections = lax.axis_size("section")
    ahead, behind = lax.rem(s + 1, sections), lax.rem(s + sections - 1, sections)

    def remote(src, dst, send, recv, to):
        return pltpu.make_async_remote_copy(
            src_ref=src, dst_ref=dst, send_sem=send, recv_sem=recv,
            device_id=to, device_id_type=MESH,
        )

    def drain(ref, sem):
        pltpu.make_async_copy(ref, ref, sem).wait()

    barrier = pltpu.get_barrier_semaphore()
    peers = [r_dev(r) for r in range(1, NR)] + [z_dev(k) for k in range(1, NZ)]
    peers += [r_dev(r, behind) for r in range(NR)] + [z_dev(k, behind) for k in (1, -1)]
    for to in peers:
        pl.semaphore_signal(barrier, inc=1, device_id=to, device_id_type=MESH)

    loads = [
        pltpu.make_async_copy(src, dst, w_sem.at[i])
        for i, (src, dst) in enumerate(
            [(act_hbm, act), (gain_hbm, gain), (ids_hbm, ids), (w1_hbm, w1), (w2_hbm, w2)]
        )
    ]
    for load in loads:
        load.start()
    for load in loads[:3]:
        load.wait()

    floats = act[...].astype(jnp.float32)
    scale = lax.rsqrt(jnp.mean(floats * floats, axis=-1, keepdims=True) + EPS)
    normed = (floats * scale * gain[...]).astype(jnp.bfloat16)
    gathered[0] = normed[:, CA:]

    i0 = lax.broadcasted_iota(jnp.int32, (tokens, tokens), 0)
    i1 = lax.broadcasted_iota(jnp.int32, (tokens, tokens), 1)
    row = ids[...]
    col = jnp.sum(jnp.where(i0 == i1, row, 0), axis=1, keepdims=True)
    rank = jnp.sum(
        jnp.where((col == row) & (i0 < i1), 1, 0), axis=0, keepdims=True
    )
    code = row * CAP + rank
    codes[0, :, 0:tokens] = jnp.broadcast_to(code, (8, tokens))

    slot = lax.broadcasted_iota(jnp.int32, (ROWS, tokens), 0)
    rel = slot // CAP
    expert_of = lax.rem(yh + rel // NX, NR // NX) * NX + lax.rem(x + lax.rem(rel, NX), NX)
    wanted = expert_of * CAP + lax.rem(slot, CAP)

    def placing(i):
        return jnp.where(wanted == codes[i, 0:1, 0:tokens], 1.0, 0.0).astype(jnp.bfloat16)

    def pack(place, rows):
        return jnp.dot(place, rows, preferred_element_type=jnp.float32).astype(jnp.bfloat16)

    def unpack(place, slots):
        return lax.dot_general(
            place, slots, (((0,), (0,)), ((), ())), preferred_element_type=jnp.float32
        )

    place_own = jnp.where(wanted == code, 1.0, 0.0).astype(jnp.bfloat16)
    packed_a[...] = pack(place_own, normed[:, :CA]).reshape(NR, CAP, CA)

    pl.semaphore_wait(barrier, len(peers))

    def ag_copy(kind, d, h, k):
        chain = CHAINS.index((d, h))
        if kind < GROUPS:
            at = pl.ds(h * CA // 2, CA // 2)
            rows = pl.ds(kind * PART, PART)
            src, dst = xa.at[ZI[d * k], rows, :, at], xa.at[ZI[d * (k + 1)], rows, :, at]
        else:
            at = pl.ds(h * cb // 2, cb // 2)
            src, dst = gathered.at[ZI[d * k], :, at], gathered.at[ZI[d * (k + 1)], :, at]
        return remote(
            src, dst, one_send.at[kind // GROUPS], ag_recv.at[kind, chain, k], z_dev(d)
        )

    def begin(kind):
        for d, h in CHAINS:
            ag_copy(kind, d, h, 0).start()

    def forward(kind, k):
        for d, h in CHAINS:
            if k <= FAR[d, h]:
                ag_copy(kind, d, h, k - 1).wait_recv()
                if k < FAR[d, h]:
                    ag_copy(kind, d, h, k).start()

    begin(2)

    for r in range(1, NR):
        remote(
            packed_a.at[r], xa.at[0, opposite(r)], one_send.at[3],
            plane_recv.at[2, r // PART], r_dev(r),
        ).start()
    xa[0, 0] = packed_a[0]
    for k in range(1, NZ):
        remote(codes.at[0], codes.at[NZ - k], one_send.at[2], one_recv.at[0], z_dev(k)).start()
    hand_act = remote(act, before, one_send.at[9], one_recv.at[3], (ahead, e))
    hand_code = remote(codes.at[0], codes.at[NZ], one_send.at[10], one_recv.at[4], (ahead, e))

    def send_packed(i, place):
        packed_b[i] = pack(place, gathered[i]).reshape(NR, CAP, cb)
        for r in range(1, NR):
            remote(
                packed_b.at[i, r], xb.at[i, opposite(r)],
                one_send.at[4], plane_recv.at[0, i], r_dev(r),
            ).start()
        xb[i, 0] = packed_b[i, 0]

    def place_of(i):
        k = [d for d in range(-3, 5) if ZI[d] == i][0]
        return placing((-k) % NZ)

    def arrive(group):
        first = max(1, group * PART)
        drain(xa.at[0, pl.ds(first, (group + 1) * PART - first)], plane_recv.at[2, group])
        begin(group)

    def packs(*blocks):
        for i in blocks:
            send_packed(i, place_of(i))

    def first_half(i, n):
        rows = n * ROWS
        for c in range(0, width, CHUNK):
            if c < CA:
                block = xa[i:i + n, :, :, c:c + CHUNK]
            else:
                block = xb[i:i + n, :, :, c - CA:c - CA + CHUNK]
            term = jnp.dot(
                block.reshape(rows, CHUNK), w1[c:c + CHUNK, :],
                preferred_element_type=jnp.float32,
            )
            if c == 0:
                pre[0:rows, :] = term
            else:
                pre[0:rows, :] += term
        return jax.nn.gelu(pre[0:rows, :], approximate=True).astype(jnp.bfloat16)

    def second_half(hidden, at):
        return jnp.dot(hidden, w2[:, at:at + CHUNK], preferred_element_type=jnp.float32)

    def returns(*blocks):
        for j in blocks:
            for r in range(1, NR):
                remote(
                    back_b.at[j, r], ret_b.at[j, opposite(r)],
                    one_send.at[5], plane_recv.at[1, j], r_dev(r),
                ).start()
            ret_b[j, 0] = back_b[j, 0]

    def run(i, n, at_once=False):
        for j in range(i, i + n):
            drain(xb.at[j, pl.ds(1, NR - 1)], plane_recv.at[0, j])
        hidden = first_half(i, n)
        for c in range(0, cb, CHUNK):
            back_b[i:i + n, :, :, c:c + CHUNK] = (
                second_half(hidden, CA + c).astype(jnp.bfloat16).reshape(n, NR, CAP, CHUNK)
            )
        if at_once:
            returns(*range(i, i + n))
        for c in range(0, CA, CHUNK):
            own_a[i:i + n, :, c:c + CHUNK] = second_half(hidden, c).reshape(n, ROWS, CHUNK)

    send_packed(0, place_own)
    hand_act.start()
    hand_code.start()
    forward(2, 1)
    arrive(0)
    drain(codes.at[pl.ds(1, NZ - 1)], one_recv.at[0])
    packs(1, 2)
    arrive(1)
    forward(2, 2)
    forward(0, 1)
    packs(3, 4)
    forward(1, 1)
    for load in loads[3:]:
        load.wait()
    run(0, 1)
    forward(2, 3)
    packs(5, 6)
    forward(0, 2)
    forward(1, 2)
    run(1, 2)
    forward(2, 4)
    packs(7)
    forward(0, 3)
    forward(1, 3)
    run(3, 2, True)
    forward(0, 4)
    forward(1, 4)

    def rs_copy(kind, d, h, k):
        chain = CHAINS.index((d, h))
        last_b = kind == GROUPS and k == 1
        if kind < GROUPS:
            src, dst = send_a.at[kind, chain, k - 1], land_a.at[kind, chain, k - 1]
        else:
            src, dst = send_b.at[chain, k - 1], land_b.at[chain, k - 1]
        return remote(
            src, dst, one_send.at[6 + kind // GROUPS], rs_recv.at[kind, chain, k - 1],
            z_dev(-d, ahead if last_b else s),
        )

    def rs_own(kind, d, h, k):
        if kind < GROUPS:
            rows = pl.ds(kind * PART * CAP, PART * CAP)
            return own_a[ZI[d * k], rows, h * CA // 2:(h + 1) * CA // 2]
        return own_b[ZI[d * k], :, h * cb // 2:(h + 1) * cb // 2]

    def rs_landed(kind, d, h, k):
        rs_copy(kind, d, h, k + 1).wait_recv()
        chain = CHAINS.index((d, h))
        land = land_a[kind, chain, k] if kind < GROUPS else land_b[chain, k]
        return land.astype(jnp.float32)

    def rs_step(kind, far, k):
        for d, h in CHAINS:
            if FAR[d, h] == far:
                total = rs_own(kind, d, h, k)
                if k < far:
                    total = total + rs_landed(kind, d, h, k)
                total = total.astype(jnp.bfloat16)
                chain = CHAINS.index((d, h))
                if kind < GROUPS:
                    send_a[kind, chain, k - 1] = total
                else:
                    send_b[chain, k - 1] = total
                rs_copy(kind, d, h, k).start()

    def rs_last(kind, h):
        return rs_landed(kind, 1, h, 0) + rs_landed(kind, -1, h, 0)

    def take_b(i):
        drain(ret_b.at[i, pl.ds(1, NR - 1)], plane_recv.at[1, i])
        own_b[i] = unpack(place_of(i), ret_b[i].reshape(ROWS, cb))

    def takes(*blocks):
        for i in blocks:
            take_b(i)

    def return_a(g):
        half = CA // 2
        for h in range(2):
            sum_a[g * PART:(g + 1) * PART, :, h * half:(h + 1) * half] = (
                rs_own(g, 1, h, 0) + rs_last(g, h)
            ).astype(jnp.bfloat16).reshape(PART, CAP, half)
        for r in range(g * PART, (g + 1) * PART):
            remote(
                sum_a.at[r], ret_a.at[opposite(r)], one_send.at[8], one_recv.at[2],
                r_dev(r, ahead),
            ).start()

    def last_b():
        tail_b[0] = own_b[0].astype(jnp.bfloat16)
        remote(tail_b.at[0], tail_b.at[1], one_send.at[11], one_recv.at[5], (ahead, e)).start()

    def write_a():
        drain(ret_a, one_recv.at[2])
        hand_act.wait_recv()
        hand_code.wait_recv()
        out[:, :CA] = (
            before[:, :CA].astype(jnp.float32)
            + unpack(placing(NZ), ret_a[...].reshape(ROWS, CA))
        ).astype(jnp.bfloat16)

    def write_b():
        drain(tail_b.at[1], one_recv.at[5])
        half = cb // 2
        for h in range(2):
            at = slice(CA + h * half, CA + (h + 1) * half)
            out[:, at] = (
                before[:, at].astype(jnp.float32)
                + tail_b[1, :, h * half:(h + 1) * half].astype(jnp.float32)
                + rs_last(GROUPS, h)
            ).astype(jnp.bfloat16)

    run(5, 2, True)
    rs_step(1, 3, 3)
    rs_step(0, 3, 3)
    run(7, 1, True)
    returns(1, 2, 0)
    rs_step(1, 4, 4)
    rs_step(0, 4, 4)
    rs_step(1, 3, 2)
    rs_step(0, 3, 2)
    rs_step(1, 4, 3)
    rs_step(0, 4, 3)
    rs_step(1, 3, 1)
    rs_step(0, 3, 1)
    takes(5, 6)
    rs_step(2, 3, 3)
    rs_step(1, 4, 2)
    rs_step(0, 4, 2)
    takes(7)
    rs_step(2, 4, 4)
    takes(3, 4)
    rs_step(2, 3, 2)
    rs_step(1, 4, 1)
    rs_step(0, 4, 1)
    rs_step(2, 4, 3)
    return_a(1)
    return_a(0)
    takes(1, 2)
    rs_step(2, 3, 1)
    rs_step(2, 4, 2)
    takes(0)
    last_b()
    rs_step(2, 4, 1)
    write_a()
    write_b()

    drain(xa.at[pl.ds(1, NZ - 1)], one_send.at[0])
    drain(gathered.at[pl.ds(1, NZ - 1)], one_send.at[1])
    drain(codes.at[pl.ds(1, NZ - 1)], one_send.at[2])
    drain(packed_a.at[pl.ds(1, NR - 1)], one_send.at[3])
    drain(packed_b.at[:, pl.ds(1, NR - 1)], one_send.at[4])
    drain(back_b.at[:, pl.ds(1, NR - 1)], one_send.at[5])
    drain(xa.at[pl.ds(1, NZ - 1)], one_send.at[6])
    drain(gathered.at[pl.ds(1, NZ - 1)], one_send.at[7])
    drain(sum_a, one_send.at[8])
    drain(tail_b.at[0], one_send.at[11])
    hand_act.wait_send()
    hand_code.wait_send()


def per_device(activations, norm_gain, in_proj, out_proj, expert_ids):
    _, tokens, width = activations.shape
    hidden = in_proj.shape[2]
    cb = width - CA
    bf16, f32 = jnp.bfloat16, jnp.float32
    vmem = pl.BlockSpec(memory_space=pltpu.VMEM)
    hbm = pl.BlockSpec(memory_space=pltpu.HBM)
    out = pl.pallas_call(
        kernel,
        out_shape=jax.ShapeDtypeStruct((tokens, width), bf16),
        in_specs=[hbm] * 5,
        out_specs=vmem,
        scratch_shapes=[
            pltpu.VMEM((tokens, width), bf16),
            pltpu.VMEM((1, width), f32),
            pltpu.VMEM((1, tokens), jnp.int32),
            pltpu.VMEM((tokens, width), bf16),
            pltpu.VMEM((width, hidden), bf16),
            pltpu.VMEM((hidden, width), bf16),
            pltpu.VMEM((NZ + 1, 8, 128), jnp.int32),
            pltpu.VMEM((NZ, tokens, cb), bf16),
            pltpu.VMEM((NR, CAP, CA), bf16),
            pltpu.VMEM((NZ, NR, CAP, cb), bf16),
            pltpu.VMEM((NZ, NR, CAP, CA), bf16),
            pltpu.VMEM((NZ, NR, CAP, cb), bf16),
            pltpu.VMEM((2 * ROWS, hidden), f32),
            pltpu.VMEM((NZ, ROWS, CA), f32),
            pltpu.VMEM((NZ, NR, CAP, cb), bf16),
            pltpu.VMEM((NZ, NR, CAP, cb), bf16),
            pltpu.VMEM((NZ, tokens, cb), f32),
            pltpu.VMEM((NR, CAP, CA), bf16),
            pltpu.VMEM((NR, CAP, CA), bf16),
            pltpu.VMEM((2, tokens, cb), bf16),
            pltpu.VMEM((GROUPS, 4, 4, PART * CAP, CA // 2), bf16),
            pltpu.VMEM((GROUPS, 4, 4, PART * CAP, CA // 2), bf16),
            pltpu.VMEM((4, 4, tokens, cb // 2), bf16),
            pltpu.VMEM((4, 4, tokens, cb // 2), bf16),
            pltpu.SemaphoreType.DMA((5,)),
            pltpu.SemaphoreType.DMA((12,)),
            pltpu.SemaphoreType.DMA((6,)),
            pltpu.SemaphoreType.DMA((GROUPS + 1, 4, 4)),
            pltpu.SemaphoreType.DMA((3, NZ)),
            pltpu.SemaphoreType.DMA((GROUPS + 1, 4, 4)),
        ],
        compiler_params=pltpu.CompilerParams(
            collective_id=0, has_side_effects=True, vmem_limit_bytes=58 * 2**20
        ),
    )(activations[0], norm_gain, expert_ids.reshape(1, tokens), in_proj[0], out_proj[0])
    return out[None]


def solution(mesh):
    return jax.shard_map(
        per_device,
        mesh=mesh,
        in_specs=(
            P("section", "expert", None),
            P("section", None),
            P("section", None, "expert"),
            P("section", "expert", None),
            P("section", "expert", None),
        ),
        out_specs=P("section", "expert", None),
        check_vma=False,
    )
```

```python
import functools

import jax
import jax.numpy as jnp
from jax import lax
from jax.experimental import pallas as pl
from jax.experimental.pallas import tpu as pltpu
from jax.sharding import PartitionSpec as P

MESH = pl.DeviceIdType.MESH
EPS = 1e-06
NZ = 8
NR = 8
NX = 4
CAP = 8
GROUPS = 2
PART = NR // GROUPS
ROWS = NR * CAP
CA = 2048
CHUNK = 1024

ZI = {0: 0, 1: 1, -1: 2, 2: 3, -2: 4, 3: 5, -3: 6, 4: 7, -4: 7}
FAR = {(1, 0): 4, (1, 1): 3, (-1, 0): 3, (-1, 1): 4}
CHAINS = [(1, 0), (-1, 1), (1, 1), (-1, 0)]


def opposite(r):
    return r // NX * NX + (NX - r % NX) % NX


def kernel(
    act_hbm, gain_hbm, ids_hbm, w1_hbm, w2_hbm, out,
    act, gain, ids, before, w1, w2, codes, gathered, packed_a, packed_b, xa, xb, pre, own_a, back_b,
    ret_b, own_b, sum_a, ret_a, tail_b,
    send_a, land_a, send_b, land_b,
    w_sem, one_send, one_recv, ag_recv, plane_recv, rs_recv,
):
    tokens, width = act_hbm.shape
    cb = width - CA
    s = lax.axis_index("section")
    e = lax.axis_index("expert")
    z, p = lax.rem(e, NZ), e // NZ
    yh, x = p // NX, lax.rem(p, NX)

    def z_dev(k, section=s):
        return (section, p * NZ + lax.rem(z + k + NZ, NZ))

    def plane_of(r):
        return lax.rem(yh + r // NX, NR // NX) * NX + lax.rem(x + r % NX, NX)

    def r_dev(r, section=s):
        return (section, plane_of(r) * NZ + z)

    sections = lax.axis_size("section")
    ahead, behind = lax.rem(s + 1, sections), lax.rem(s + sections - 1, sections)

    def remote(src, dst, send, recv, to):
        return pltpu.make_async_remote_copy(
            src_ref=src, dst_ref=dst, send_sem=send, recv_sem=recv,
            device_id=to, device_id_type=MESH,
        )

    def drain(ref, sem):
        pltpu.make_async_copy(ref, ref, sem).wait()

    barrier = pltpu.get_barrier_semaphore()
    peers = [r_dev(r) for r in range(1, NR)] + [z_dev(k) for k in range(1, NZ)]
    peers += [r_dev(r, behind) for r in range(NR)] + [z_dev(k, behind) for k in (1, -1)]
    for to in peers:
        pl.semaphore_signal(barrier, inc=1, device_id=to, device_id_type=MESH)

    loads = [
        pltpu.make_async_copy(src, dst, w_sem.at[i])
        for i, (src, dst) in enumerate(
            [(act_hbm, act), (gain_hbm, gain), (ids_hbm, ids), (w1_hbm, w1), (w2_hbm, w2)]
        )
    ]
    for load in loads:
        load.start()
    for load in loads[:3]:
        load.wait()

    floats = act[...].astype(jnp.float32)
    scale = lax.rsqrt(jnp.mean(floats * floats, axis=-1, keepdims=True) + EPS)
    normed = (floats * scale * gain[...]).astype(jnp.bfloat16)
    gathered[0] = normed[:, CA:]

    i0 = lax.broadcasted_iota(jnp.int32, (tokens, tokens), 0)
    i1 = lax.broadcasted_iota(jnp.int32, (tokens, tokens), 1)
    row = ids[...]
    col = jnp.sum(jnp.where(i0 == i1, row, 0), axis=1, keepdims=True)
    rank = jnp.sum(
        jnp.where((col == row) & (i0 < i1), 1, 0), axis=0, keepdims=True
    )
    code = row * CAP + rank
    codes[0, :, 0:tokens] = jnp.broadcast_to(code, (8, tokens))

    slot = lax.broadcasted_iota(jnp.int32, (ROWS, tokens), 0)
    rel = slot // CAP
    expert_of = lax.rem(yh + rel // NX, NR // NX) * NX + lax.rem(x + lax.rem(rel, NX), NX)
    wanted = expert_of * CAP + lax.rem(slot, CAP)

    def placing(i):
        return jnp.where(wanted == codes[i, 0:1, 0:tokens], 1.0, 0.0).astype(jnp.bfloat16)

    def pack(place, rows):
        return jnp.dot(place, rows, preferred_element_type=jnp.float32).astype(jnp.bfloat16)

    def unpack(place, slots):
        return lax.dot_general(
            place, slots, (((0,), (0,)), ((), ())), preferred_element_type=jnp.float32
        )

    place_own = jnp.where(wanted == code, 1.0, 0.0).astype(jnp.bfloat16)
    packed_a[...] = pack(place_own, normed[:, :CA]).reshape(NR, CAP, CA)

    pl.semaphore_wait(barrier, len(peers))

    def ag_copy(kind, d, h, k):
        chain = CHAINS.index((d, h))
        if kind < GROUPS:
            at = pl.ds(h * CA // 2, CA // 2)
            rows = pl.ds(kind * PART, PART)
            src, dst = xa.at[ZI[d * k], rows, :, at], xa.at[ZI[d * (k + 1)], rows, :, at]
        else:
            at = pl.ds(h * cb // 2, cb // 2)
            src, dst = gathered.at[ZI[d * k], :, at], gathered.at[ZI[d * (k + 1)], :, at]
        return remote(
            src, dst, one_send.at[kind // GROUPS], ag_recv.at[kind, chain, k], z_dev(d)
        )

    def begin(kind):
        for d, h in CHAINS:
            ag_copy(kind, d, h, 0).start()

    def forward(kind, k, far):
        for d, h in CHAINS:
            if FAR[d, h] == far:
                ag_copy(kind, d, h, k - 1).wait_recv()
                if k < far:
                    ag_copy(kind, d, h, k).start()

    begin(2)

    for r in range(1, NR):
        remote(
            packed_a.at[r], xa.at[0, opposite(r)], one_send.at[3],
            plane_recv.at[2, r // PART], r_dev(r),
        ).start()
    xa[0, 0] = packed_a[0]
    for k in range(1, NZ):
        remote(codes.at[0], codes.at[NZ - k], one_send.at[2], one_recv.at[0], z_dev(k)).start()
    hand_act = remote(act, before, one_send.at[9], one_recv.at[3], (ahead, e))
    hand_code = remote(codes.at[0], codes.at[NZ], one_send.at[10], one_recv.at[4], (ahead, e))

    def send_packed(i, place):
        packed_b[i] = pack(place, gathered[i]).reshape(NR, CAP, cb)
        for r in range(1, NR):
            remote(
                packed_b.at[i, r], xb.at[i, opposite(r)],
                one_send.at[4], plane_recv.at[0, i], r_dev(r),
            ).start()
        xb[i, 0] = packed_b[i, 0]

    def place_of(i):
        k = [d for d in range(-3, 5) if ZI[d] == i][0]
        return placing((-k) % NZ)

    def arrive(group):
        first = max(1, group * PART)
        drain(xa.at[0, pl.ds(first, (group + 1) * PART - first)], plane_recv.at[2, group])
        begin(group)

    def packs(*blocks):
        for i in blocks:
            send_packed(i, place_of(i))

    def hidden_of(i, j, a=0, b=NR):
        rows = (j - i) * (b - a) * CAP
        for c in range(0, width, CHUNK):
            if c < CA:
                block = xa[i:j, a:b, :, c:c + CHUNK]
            else:
                block = xb[i:j, a:b, :, c - CA:c - CA + CHUNK]
            term = jnp.dot(
                block.reshape(rows, CHUNK), w1[c:c + CHUNK, :],
                preferred_element_type=jnp.float32,
            )
            if c == 0:
                pre[0:rows, :] = term
            else:
                pre[0:rows, :] += term
        return jax.nn.gelu(pre[0:rows, :], approximate=True).astype(jnp.bfloat16)

    def part_of(hidden, at):
        return jnp.dot(hidden, w2[:, at:at + CHUNK], preferred_element_type=jnp.float32)

    def columns_b(hidden, i, j, a=0, b=NR):
        for c in range(0, cb, CHUNK):
            back_b[i:j, a:b, :, c:c + CHUNK] = (
                part_of(hidden, CA + c).astype(jnp.bfloat16).reshape(j - i, b - a, CAP, CHUNK)
            )

    def columns_a(hidden, i, j, a=0, b=NR):
        for c in range(0, CA, CHUNK):
            own_a[i:j, a * CAP:b * CAP, c:c + CHUNK] = (
                part_of(hidden, c).reshape(j - i, (b - a) * CAP, CHUNK)
            )

    def returns(j, a, b):
        for r in range(a, b):
            if r == 0:
                ret_b[j, 0] = back_b[j, 0]
            else:
                remote(
                    back_b.at[j, r], ret_b.at[j, opposite(r)],
                    one_send.at[5], plane_recv.at[1, j], r_dev(r),
                ).start()

    def landed(*blocks):
        for j in blocks:
            drain(xb.at[j, pl.ds(1, NR - 1)], plane_recv.at[0, j])

    def rs_copy(kind, d, h, k):
        chain = CHAINS.index((d, h))
        last_b = kind == GROUPS and k == 1
        if kind < GROUPS:
            src, dst = send_a.at[kind, chain, k - 1], land_a.at[kind, chain, k - 1]
        else:
            src, dst = send_b.at[chain, k - 1], land_b.at[chain, k - 1]
        return remote(
            src, dst, one_send.at[6 + kind // GROUPS], rs_recv.at[kind, chain, k - 1],
            z_dev(-d, ahead if last_b else s),
        )

    def rs_own(kind, d, h, k):
        if kind < GROUPS:
            rows = pl.ds(kind * PART * CAP, PART * CAP)
            return own_a[ZI[d * k], rows, h * CA // 2:(h + 1) * CA // 2]
        return own_b[ZI[d * k], :, h * cb // 2:(h + 1) * cb // 2]

    def rs_landed(kind, d, h, k):
        rs_copy(kind, d, h, k + 1).wait_recv()
        chain = CHAINS.index((d, h))
        land = land_a[kind, chain, k] if kind < GROUPS else land_b[chain, k]
        return land.astype(jnp.float32)

    def rs_step(kind, far, k):
        for d, h in CHAINS:
            if FAR[d, h] == far:
                total = rs_own(kind, d, h, k)
                if k < far:
                    total = total + rs_landed(kind, d, h, k)
                total = total.astype(jnp.bfloat16)
                chain = CHAINS.index((d, h))
                if kind < GROUPS:
                    send_a[kind, chain, k - 1] = total
                else:
                    send_b[chain, k - 1] = total
                rs_copy(kind, d, h, k).start()

    def rs_last(kind, h):
        return rs_landed(kind, 1, h, 0) + rs_landed(kind, -1, h, 0)

    def take_b(i):
        drain(ret_b.at[i, pl.ds(1, NR - 1)], plane_recv.at[1, i])
        own_b[i] = unpack(place_of(i), ret_b[i].reshape(ROWS, cb))

    def return_a(g):
        half = CA // 2
        for h in range(2):
            sum_a[g * PART:(g + 1) * PART, :, h * half:(h + 1) * half] = (
                rs_own(g, 1, h, 0) + rs_last(g, h)
            ).astype(jnp.bfloat16).reshape(PART, CAP, half)
        for r in range(g * PART, (g + 1) * PART):
            remote(
                sum_a.at[r], ret_a.at[opposite(r)], one_send.at[8], one_recv.at[2],
                r_dev(r, ahead),
            ).start()

    def last_b():
        tail_b[0] = own_b[0].astype(jnp.bfloat16)
        remote(tail_b.at[0], tail_b.at[1], one_send.at[11], one_recv.at[5], (ahead, e)).start()

    def write_a():
        drain(ret_a, one_recv.at[2])
        hand_act.wait_recv()
        hand_code.wait_recv()
        out[:, :CA] = (
            before[:, :CA].astype(jnp.float32)
            + unpack(placing(NZ), ret_a[...].reshape(ROWS, CA))
        ).astype(jnp.bfloat16)

    def write_b():
        drain(tail_b.at[1], one_recv.at[5])
        half = cb // 2
        for h in range(2):
            at = slice(CA + h * half, CA + (h + 1) * half)
            out[:, at] = (
                before[:, at].astype(jnp.float32)
                + tail_b[1, :, h * half:(h + 1) * half].astype(jnp.float32)
                + rs_last(GROUPS, h)
            ).astype(jnp.bfloat16)

    send_packed(0, place_own)
    hand_act.start()
    hand_code.start()
    forward(2, 1, 4)
    forward(2, 1, 3)
    drain(codes.at[pl.ds(1, NZ - 1)], one_recv.at[0])
    arrive(0)
    packs(2)
    forward(2, 2, 3)
    forward(2, 2, 4)
    packs(4)
    arrive(1)
    packs(3)
    forward(2, 3, 4)
    forward(2, 3, 3)
    packs(6)
    forward(1, 1, 4)
    forward(0, 1, 3)
    forward(0, 1, 4)
    packs(5)
    forward(2, 4, 4)
    for load in loads[3:]:
        load.wait()
    landed(0)
    h0101 = hidden_of(0, 1, 0, NR)
    packs(7)
    forward(1, 2, 4)
    forward(1, 1, 3)
    columns_b(h0101, 0, 1, 0, NR)
    packs(1)
    forward(0, 2, 4)
    forward(1, 3, 4)
    forward(1, 2, 3)
    returns(0, 0, PART)
    forward(0, 2, 3)
    landed(3, 4)
    h3501 = hidden_of(3, 5, 0, NR)
    columns_b(h3501, 3, 5, 0, NR)
    forward(0, 3, 4)
    returns(3, PART, NR)
    returns(3, 0, PART)
    forward(1, 4, 4)
    returns(0, PART, NR)
    forward(1, 3, 3)
    landed(5, 6, 7)
    h581 = hidden_of(5, 8, PART, NR)
    columns_a(h581, 5, 8, PART, NR)
    rs_step(1, 4, 4)
    rs_step(1, 3, 3)
    forward(0, 4, 4)
    returns(4, PART, NR)
    forward(0, 3, 3)
    h580 = hidden_of(5, 8, 0, PART)
    columns_a(h580, 5, 8, 0, PART)
    rs_step(0, 4, 4)
    columns_b(h581, 5, 8, PART, NR)
    rs_step(0, 3, 3)
    columns_b(h580, 5, 8, 0, PART)
    returns(5, 0, PART)
    returns(7, PART, NR)
    returns(7, 0, PART)
    rs_step(1, 4, 3)
    rs_step(0, 4, 3)
    returns(6, PART, NR)
    columns_a(h3501, 3, 5, 0, NR)
    rs_step(1, 3, 2)
    returns(6, 0, PART)
    rs_step(0, 3, 2)
    take_b(3)
    rs_step(1, 4, 2)
    landed(1, 2)
    h1301 = hidden_of(1, 3, 0, NR)
    returns(5, PART, NR)
    columns_b(h1301, 1, 3, 0, NR)
    returns(1, PART, NR)
    rs_step(0, 4, 2)
    returns(4, 0, PART)
    returns(1, 0, PART)
    columns_a(h1301, 1, 3, 0, NR)
    returns(2, PART, NR)
    rs_step(1, 3, 1)
    take_b(7)
    rs_step(1, 4, 1)
    rs_step(2, 4, 4)
    take_b(0)
    take_b(6)
    rs_step(0, 3, 1)
    returns(2, 0, PART)
    take_b(5)
    rs_step(2, 3, 3)
    columns_a(h0101, 0, 1, 0, NR)
    rs_step(2, 4, 3)
    return_a(1)
    last_b()
    take_b(4)
    rs_step(0, 4, 1)
    rs_step(2, 3, 2)
    take_b(1)
    rs_step(2, 4, 2)
    return_a(0)
    take_b(2)
    rs_step(2, 3, 1)
    rs_step(2, 4, 1)
    write_a()
    write_b()

    drain(xa.at[pl.ds(1, NZ - 1)], one_send.at[0])
    drain(gathered.at[pl.ds(1, NZ - 1)], one_send.at[1])
    drain(codes.at[pl.ds(1, NZ - 1)], one_send.at[2])
    drain(packed_a.at[pl.ds(1, NR - 1)], one_send.at[3])
    drain(packed_b.at[:, pl.ds(1, NR - 1)], one_send.at[4])
    drain(back_b.at[:, pl.ds(1, NR - 1)], one_send.at[5])
    drain(xa.at[pl.ds(1, NZ - 1)], one_send.at[6])
    drain(gathered.at[pl.ds(1, NZ - 1)], one_send.at[7])
    drain(sum_a, one_send.at[8])
    drain(tail_b.at[0], one_send.at[11])
    hand_act.wait_send()
    hand_code.wait_send()


def per_device(activations, norm_gain, in_proj, out_proj, expert_ids):
    _, tokens, width = activations.shape
    hidden = in_proj.shape[2]
    cb = width - CA
    bf16, f32 = jnp.bfloat16, jnp.float32
    vmem = pl.BlockSpec(memory_space=pltpu.VMEM)
    hbm = pl.BlockSpec(memory_space=pltpu.HBM)
    out = pl.pallas_call(
        kernel,
        out_shape=jax.ShapeDtypeStruct((tokens, width), bf16),
        in_specs=[hbm] * 5,
        out_specs=vmem,
        scratch_shapes=[
            pltpu.VMEM((tokens, width), bf16),
            pltpu.VMEM((1, width), f32),
            pltpu.VMEM((1, tokens), jnp.int32),
            pltpu.VMEM((tokens, width), bf16),
            pltpu.VMEM((width, hidden), bf16),
            pltpu.VMEM((hidden, width), bf16),
            pltpu.VMEM((NZ + 1, 8, 128), jnp.int32),
            pltpu.VMEM((NZ, tokens, cb), bf16),
            pltpu.VMEM((NR, CAP, CA), bf16),
            pltpu.VMEM((NZ, NR, CAP, cb), bf16),
            pltpu.VMEM((NZ, NR, CAP, CA), bf16),
            pltpu.VMEM((NZ, NR, CAP, cb), bf16),
            pltpu.VMEM((2 * ROWS, hidden), f32),
            pltpu.VMEM((NZ, ROWS, CA), f32),
            pltpu.VMEM((NZ, NR, CAP, cb), bf16),
            pltpu.VMEM((NZ, NR, CAP, cb), bf16),
            pltpu.VMEM((NZ, tokens, cb), f32),
            pltpu.VMEM((NR, CAP, CA), bf16),
            pltpu.VMEM((NR, CAP, CA), bf16),
            pltpu.VMEM((2, tokens, cb), bf16),
            pltpu.VMEM((GROUPS, 4, 4, PART * CAP, CA // 2), bf16),
            pltpu.VMEM((GROUPS, 4, 4, PART * CAP, CA // 2), bf16),
            pltpu.VMEM((4, 4, tokens, cb // 2), bf16),
            pltpu.VMEM((4, 4, tokens, cb // 2), bf16),
            pltpu.SemaphoreType.DMA((5,)),
            pltpu.SemaphoreType.DMA((12,)),
            pltpu.SemaphoreType.DMA((6,)),
            pltpu.SemaphoreType.DMA((GROUPS + 1, 4, 4)),
            pltpu.SemaphoreType.DMA((3, NZ)),
            pltpu.SemaphoreType.DMA((GROUPS + 1, 4, 4)),
        ],
        compiler_params=pltpu.CompilerParams(
            collective_id=0, has_side_effects=True, vmem_limit_bytes=58 * 2**20
        ),
    )(activations[0], norm_gain, expert_ids.reshape(1, tokens), in_proj[0], out_proj[0])
    return out[None]


def solution(mesh):
    return jax.shard_map(
        per_device,
        mesh=mesh,
        in_specs=(
            P("section", "expert", None),
            P("section", None),
            P("section", None, "expert"),
            P("section", "expert", None),
            P("section", "expert", None),
        ),
        out_specs=P("section", "expert", None),
        check_vma=False,
    )
```

```python
import functools

import jax
import jax.numpy as jnp
from jax import lax
from jax.experimental import pallas as pl
from jax.experimental.pallas import tpu as pltpu
from jax.sharding import PartitionSpec as P

MESH = pl.DeviceIdType.MESH
EPS = 1e-06
NZ = 8
NR = 8
NX = 4
CAP = 8
GROUPS = 2
PART = NR // GROUPS
ROWS = NR * CAP
CA = 2048
CHUNK = 1024

ZI = {0: 0, 1: 1, -1: 2, 2: 3, -2: 4, 3: 5, -3: 6, 4: 7, -4: 7}
FAR = {(1, 0): 4, (1, 1): 3, (-1, 0): 3, (-1, 1): 4}
CHAINS = [(1, 0), (-1, 1), (1, 1), (-1, 0)]


def opposite(r):
    return r // NX * NX + (NX - r % NX) % NX


def kernel(
    act_hbm, gain_hbm, ids_hbm, w1_hbm, w2_hbm, out,
    act, gain, ids, before, w1, w2, codes, gathered, packed_a, packed_b, xa, xb, pre, own_a, back_b,
    ret_b, own_b, sum_a, ret_a, tail_b,
    send_a, land_a, send_b, land_b,
    w_sem, one_send, one_recv, ag_recv, plane_recv, rs_recv,
):
    tokens, width = act_hbm.shape
    cb = width - CA
    s = lax.axis_index("section")
    e = lax.axis_index("expert")
    z, p = lax.rem(e, NZ), e // NZ
    yh, x = p // NX, lax.rem(p, NX)

    def z_dev(k, section=s):
        return (section, p * NZ + lax.rem(z + k + NZ, NZ))

    def plane_of(r):
        return lax.rem(yh + r // NX, NR // NX) * NX + lax.rem(x + r % NX, NX)

    def r_dev(r, section=s):
        return (section, plane_of(r) * NZ + z)

    sections = lax.axis_size("section")
    ahead, behind = lax.rem(s + 1, sections), lax.rem(s + sections - 1, sections)

    def remote(src, dst, send, recv, to):
        return pltpu.make_async_remote_copy(
            src_ref=src, dst_ref=dst, send_sem=send, recv_sem=recv,
            device_id=to, device_id_type=MESH,
        )

    def drain(ref, sem):
        pltpu.make_async_copy(ref, ref, sem).wait()

    barrier = pltpu.get_barrier_semaphore()
    peers = [r_dev(r) for r in range(1, NR)] + [z_dev(k) for k in range(1, NZ)]
    peers += [r_dev(r, behind) for r in range(NR)] + [z_dev(k, behind) for k in (1, -1)]
    for to in peers:
        pl.semaphore_signal(barrier, inc=1, device_id=to, device_id_type=MESH)

    loads = [
        pltpu.make_async_copy(src, dst, w_sem.at[i])
        for i, (src, dst) in enumerate(
            [(act_hbm, act), (gain_hbm, gain), (ids_hbm, ids), (w1_hbm, w1), (w2_hbm, w2)]
        )
    ]
    for load in loads:
        load.start()
    for load in loads[:3]:
        load.wait()

    floats = act[...].astype(jnp.float32)
    scale = lax.rsqrt(jnp.mean(floats * floats, axis=-1, keepdims=True) + EPS)
    normed = (floats * scale * gain[...]).astype(jnp.bfloat16)
    gathered[0] = normed[:, CA:]

    i0 = lax.broadcasted_iota(jnp.int32, (tokens, tokens), 0)
    i1 = lax.broadcasted_iota(jnp.int32, (tokens, tokens), 1)
    row = ids[...]
    col = jnp.sum(jnp.where(i0 == i1, row, 0), axis=1, keepdims=True)
    rank = jnp.sum(
        jnp.where((col == row) & (i0 < i1), 1, 0), axis=0, keepdims=True
    )
    code = row * CAP + rank
    codes[0, :, 0:tokens] = jnp.broadcast_to(code, (8, tokens))

    slot = lax.broadcasted_iota(jnp.int32, (ROWS, tokens), 0)
    rel = slot // CAP
    expert_of = lax.rem(yh + rel // NX, NR // NX) * NX + lax.rem(x + lax.rem(rel, NX), NX)
    wanted = expert_of * CAP + lax.rem(slot, CAP)

    def placing(i):
        return jnp.where(wanted == codes[i, 0:1, 0:tokens], 1.0, 0.0).astype(jnp.bfloat16)

    def pack(place, rows):
        return jnp.dot(place, rows, preferred_element_type=jnp.float32).astype(jnp.bfloat16)

    def unpack(place, slots):
        return lax.dot_general(
            place, slots, (((0,), (0,)), ((), ())), preferred_element_type=jnp.float32
        )

    place_own = jnp.where(wanted == code, 1.0, 0.0).astype(jnp.bfloat16)
    packed_a[...] = pack(place_own, normed[:, :CA]).reshape(NR, CAP, CA)

    pl.semaphore_wait(barrier, len(peers))

    def ag_copy(kind, d, h, k):
        chain = CHAINS.index((d, h))
        if kind < GROUPS:
            at = pl.ds(h * CA // 2, CA // 2)
            rows = pl.ds(kind * PART, PART)
            src, dst = xa.at[ZI[d * k], rows, :, at], xa.at[ZI[d * (k + 1)], rows, :, at]
        else:
            at = pl.ds(h * cb // 2, cb // 2)
            src, dst = gathered.at[ZI[d * k], :, at], gathered.at[ZI[d * (k + 1)], :, at]
        return remote(
            src, dst, one_send.at[kind // GROUPS], ag_recv.at[kind, chain, k], z_dev(d)
        )

    def begin(kind):
        for d, h in CHAINS:
            ag_copy(kind, d, h, 0).start()

    def forward(kind, k, far):
        for d, h in CHAINS:
            if FAR[d, h] == far:
                ag_copy(kind, d, h, k - 1).wait_recv()
                if k < far:
                    ag_copy(kind, d, h, k).start()

    begin(2)

    for r in range(1, NR):
        remote(
            packed_a.at[r], xa.at[0, opposite(r)], one_send.at[3],
            plane_recv.at[2, r // PART], r_dev(r),
        ).start()
    xa[0, 0] = packed_a[0]
    for k in range(1, NZ):
        remote(codes.at[0], codes.at[NZ - k], one_send.at[2], one_recv.at[0], z_dev(k)).start()
    hand_act = remote(act, before, one_send.at[9], one_recv.at[3], (ahead, e))
    hand_code = remote(codes.at[0], codes.at[NZ], one_send.at[10], one_recv.at[4], (ahead, e))

    def send_packed(i, place):
        packed_b[i] = pack(place, gathered[i]).reshape(NR, CAP, cb)
        for r in range(1, NR):
            remote(
                packed_b.at[i, r], xb.at[i, opposite(r)],
                one_send.at[4], plane_recv.at[0, i], r_dev(r),
            ).start()
        xb[i, 0] = packed_b[i, 0]

    def place_of(i):
        k = [d for d in range(-3, 5) if ZI[d] == i][0]
        return placing((-k) % NZ)

    def arrive(group):
        first = max(1, group * PART)
        drain(xa.at[0, pl.ds(first, (group + 1) * PART - first)], plane_recv.at[2, group])
        begin(group)

    def packs(*blocks):
        for i in blocks:
            send_packed(i, place_of(i))

    def hidden_of(i, j, a=0, b=NR):
        rows = (j - i) * (b - a) * CAP
        for c in range(0, width, CHUNK):
            if c < CA:
                block = xa[i:j, a:b, :, c:c + CHUNK]
            else:
                block = xb[i:j, a:b, :, c - CA:c - CA + CHUNK]
            term = jnp.dot(
                block.reshape(rows, CHUNK), w1[c:c + CHUNK, :],
                preferred_element_type=jnp.float32,
            )
            if c == 0:
                pre[0:rows, :] = term
            else:
                pre[0:rows, :] += term
        return jax.nn.gelu(pre[0:rows, :], approximate=True).astype(jnp.bfloat16)

    def part_of(hidden, at):
        return jnp.dot(hidden, w2[:, at:at + CHUNK], preferred_element_type=jnp.float32)

    def columns_b(hidden, i, j, a=0, b=NR):
        for c in range(0, cb, CHUNK):
            back_b[i:j, a:b, :, c:c + CHUNK] = (
                part_of(hidden, CA + c).astype(jnp.bfloat16).reshape(j - i, b - a, CAP, CHUNK)
            )

    def columns_a(hidden, i, j, a=0, b=NR):
        for c in range(0, CA, CHUNK):
            own_a[i:j, a * CAP:b * CAP, c:c + CHUNK] = (
                part_of(hidden, c).reshape(j - i, (b - a) * CAP, CHUNK)
            )

    def returns(j, a, b):
        for r in range(a, b):
            if r == 0:
                ret_b[j, 0] = back_b[j, 0]
            else:
                remote(
                    back_b.at[j, r], ret_b.at[j, opposite(r)],
                    one_send.at[5], plane_recv.at[1, j], r_dev(r),
                ).start()

    def landed(*blocks):
        for j in blocks:
            drain(xb.at[j, pl.ds(1, NR - 1)], plane_recv.at[0, j])

    def rs_copy(kind, d, h, k):
        chain = CHAINS.index((d, h))
        last_b = kind == GROUPS and k == 1
        if kind < GROUPS:
            src, dst = send_a.at[kind, chain, k - 1], land_a.at[kind, chain, k - 1]
        else:
            src, dst = send_b.at[chain, k - 1], land_b.at[chain, k - 1]
        return remote(
            src, dst, one_send.at[6 + kind // GROUPS], rs_recv.at[kind, chain, k - 1],
            z_dev(-d, ahead if last_b else s),
        )

    def rs_own(kind, d, h, k):
        if kind < GROUPS:
            rows = pl.ds(kind * PART * CAP, PART * CAP)
            return own_a[ZI[d * k], rows, h * CA // 2:(h + 1) * CA // 2]
        return own_b[ZI[d * k], :, h * cb // 2:(h + 1) * cb // 2]

    def rs_landed(kind, d, h, k):
        rs_copy(kind, d, h, k + 1).wait_recv()
        chain = CHAINS.index((d, h))
        land = land_a[kind, chain, k] if kind < GROUPS else land_b[chain, k]
        return land.astype(jnp.float32)

    def rs_step(kind, far, k):
        for d, h in CHAINS:
            if FAR[d, h] == far:
                total = rs_own(kind, d, h, k)
                if k < far:
                    total = total + rs_landed(kind, d, h, k)
                total = total.astype(jnp.bfloat16)
                chain = CHAINS.index((d, h))
                if kind < GROUPS:
                    send_a[kind, chain, k - 1] = total
                else:
                    send_b[chain, k - 1] = total
                rs_copy(kind, d, h, k).start()

    def rs_last(kind, h):
        return rs_landed(kind, 1, h, 0) + rs_landed(kind, -1, h, 0)

    def take_b(i):
        drain(ret_b.at[i, pl.ds(1, NR - 1)], plane_recv.at[1, i])
        own_b[i] = unpack(place_of(i), ret_b[i].reshape(ROWS, cb))

    def return_a(g):
        half = CA // 2
        for h in range(2):
            sum_a[g * PART:(g + 1) * PART, :, h * half:(h + 1) * half] = (
                rs_own(g, 1, h, 0) + rs_last(g, h)
            ).astype(jnp.bfloat16).reshape(PART, CAP, half)
        for r in range(g * PART, (g + 1) * PART):
            remote(
                sum_a.at[r], ret_a.at[opposite(r)], one_send.at[8], one_recv.at[2],
                r_dev(r, ahead),
            ).start()

    def last_b():
        tail_b[0] = own_b[0].astype(jnp.bfloat16)
        remote(tail_b.at[0], tail_b.at[1], one_send.at[11], one_recv.at[5], (ahead, e)).start()

    def write_a():
        drain(ret_a, one_recv.at[2])
        hand_act.wait_recv()
        hand_code.wait_recv()
        out[:, :CA] = (
            before[:, :CA].astype(jnp.float32)
            + unpack(placing(NZ), ret_a[...].reshape(ROWS, CA))
        ).astype(jnp.bfloat16)

    def write_b():
        drain(tail_b.at[1], one_recv.at[5])
        half = cb // 2
        for h in range(2):
            at = slice(CA + h * half, CA + (h + 1) * half)
            out[:, at] = (
                before[:, at].astype(jnp.float32)
                + tail_b[1, :, h * half:(h + 1) * half].astype(jnp.float32)
                + rs_last(GROUPS, h)
            ).astype(jnp.bfloat16)

    send_packed(0, place_own)
    forward(2, 1, 4)
    forward(2, 1, 3)
    drain(codes.at[pl.ds(1, NZ - 1)], one_recv.at[0])
    arrive(0)
    packs(2)
    forward(2, 2, 3)
    forward(2, 2, 4)
    packs(4)
    arrive(1)
    packs(3)
    forward(2, 3, 4)
    forward(2, 3, 3)
    packs(6)
    forward(1, 1, 4)
    forward(0, 1, 3)
    forward(0, 1, 4)
    packs(5)
    forward(2, 4, 4)
    for load in loads[3:]:
        load.wait()
    landed(0)
    h0101 = hidden_of(0, 1, 0, NR)
    packs(7)
    hand_act.start()
    hand_code.start()
    forward(1, 2, 4)
    forward(1, 1, 3)
    columns_b(h0101, 0, 1, 0, NR)
    packs(1)
    forward(0, 2, 4)
    forward(1, 3, 4)
    forward(1, 2, 3)
    returns(0, 0, PART)
    forward(0, 2, 3)
    landed(3, 4)
    h3501 = hidden_of(3, 5, 0, NR)
    columns_b(h3501, 3, 5, 0, NR)
    forward(0, 3, 4)
    returns(3, PART, NR)
    returns(3, 0, PART)
    forward(1, 4, 4)
    returns(0, PART, NR)
    forward(1, 3, 3)
    landed(5, 6, 7)
    h581 = hidden_of(5, 8, PART, NR)
    columns_a(h581, 5, 8, PART, NR)
    rs_step(1, 4, 4)
    rs_step(1, 3, 3)
    forward(0, 4, 4)
    returns(4, PART, NR)
    forward(0, 3, 3)
    h580 = hidden_of(5, 8, 0, PART)
    columns_a(h580, 5, 8, 0, PART)
    rs_step(0, 4, 4)
    columns_b(h581, 5, 8, PART, NR)
    rs_step(0, 3, 3)
    columns_b(h580, 5, 8, 0, PART)
    returns(5, 0, PART)
    returns(7, PART, NR)
    returns(7, 0, PART)
    rs_step(1, 4, 3)
    rs_step(0, 4, 3)
    returns(6, PART, NR)
    columns_a(h3501, 3, 5, 0, NR)
    rs_step(1, 3, 2)
    returns(6, 0, PART)
    rs_step(0, 3, 2)
    take_b(3)
    rs_step(1, 4, 2)
    landed(1, 2)
    h1301 = hidden_of(1, 3, 0, NR)
    returns(5, PART, NR)
    columns_b(h1301, 1, 3, 0, NR)
    returns(1, PART, NR)
    rs_step(0, 4, 2)
    returns(4, 0, PART)
    returns(1, 0, PART)
    columns_a(h1301, 1, 3, 0, NR)
    returns(2, PART, NR)
    rs_step(1, 3, 1)
    take_b(7)
    rs_step(1, 4, 1)
    rs_step(2, 4, 4)
    take_b(0)
    take_b(6)
    rs_step(0, 3, 1)
    returns(2, 0, PART)
    take_b(5)
    rs_step(2, 3, 3)
    columns_a(h0101, 0, 1, 0, NR)
    rs_step(2, 4, 3)
    return_a(1)
    last_b()
    take_b(4)
    rs_step(0, 4, 1)
    rs_step(2, 3, 2)
    take_b(1)
    rs_step(2, 4, 2)
    return_a(0)
    take_b(2)
    rs_step(2, 3, 1)
    rs_step(2, 4, 1)
    write_a()
    write_b()

    drain(xa.at[pl.ds(1, NZ - 1)], one_send.at[0])
    drain(gathered.at[pl.ds(1, NZ - 1)], one_send.at[1])
    drain(codes.at[pl.ds(1, NZ - 1)], one_send.at[2])
    drain(packed_a.at[pl.ds(1, NR - 1)], one_send.at[3])
    drain(packed_b.at[:, pl.ds(1, NR - 1)], one_send.at[4])
    drain(back_b.at[:, pl.ds(1, NR - 1)], one_send.at[5])
    drain(xa.at[pl.ds(1, NZ - 1)], one_send.at[6])
    drain(gathered.at[pl.ds(1, NZ - 1)], one_send.at[7])
    drain(sum_a, one_send.at[8])
    drain(tail_b.at[0], one_send.at[11])
    hand_act.wait_send()
    hand_code.wait_send()


def per_device(activations, norm_gain, in_proj, out_proj, expert_ids):
    _, tokens, width = activations.shape
    hidden = in_proj.shape[2]
    cb = width - CA
    bf16, f32 = jnp.bfloat16, jnp.float32
    vmem = pl.BlockSpec(memory_space=pltpu.VMEM)
    hbm = pl.BlockSpec(memory_space=pltpu.HBM)
    out = pl.pallas_call(
        kernel,
        out_shape=jax.ShapeDtypeStruct((tokens, width), bf16),
        in_specs=[hbm] * 5,
        out_specs=vmem,
        scratch_shapes=[
            pltpu.VMEM((tokens, width), bf16),
            pltpu.VMEM((1, width), f32),
            pltpu.VMEM((1, tokens), jnp.int32),
            pltpu.VMEM((tokens, width), bf16),
            pltpu.VMEM((width, hidden), bf16),
            pltpu.VMEM((hidden, width), bf16),
            pltpu.VMEM((NZ + 1, 8, 128), jnp.int32),
            pltpu.VMEM((NZ, tokens, cb), bf16),
            pltpu.VMEM((NR, CAP, CA), bf16),
            pltpu.VMEM((NZ, NR, CAP, cb), bf16),
            pltpu.VMEM((NZ, NR, CAP, CA), bf16),
            pltpu.VMEM((NZ, NR, CAP, cb), bf16),
            pltpu.VMEM((2 * ROWS, hidden), f32),
            pltpu.VMEM((NZ, ROWS, CA), f32),
            pltpu.VMEM((NZ, NR, CAP, cb), bf16),
            pltpu.VMEM((NZ, NR, CAP, cb), bf16),
            pltpu.VMEM((NZ, tokens, cb), f32),
            pltpu.VMEM((NR, CAP, CA), bf16),
            pltpu.VMEM((NR, CAP, CA), bf16),
            pltpu.VMEM((2, tokens, cb), bf16),
            pltpu.VMEM((GROUPS, 4, 4, PART * CAP, CA // 2), bf16),
            pltpu.VMEM((GROUPS, 4, 4, PART * CAP, CA // 2), bf16),
            pltpu.VMEM((4, 4, tokens, cb // 2), bf16),
            pltpu.VMEM((4, 4, tokens, cb // 2), bf16),
            pltpu.SemaphoreType.DMA((5,)),
            pltpu.SemaphoreType.DMA((12,)),
            pltpu.SemaphoreType.DMA((6,)),
            pltpu.SemaphoreType.DMA((GROUPS + 1, 4, 4)),
            pltpu.SemaphoreType.DMA((3, NZ)),
            pltpu.SemaphoreType.DMA((GROUPS + 1, 4, 4)),
        ],
        compiler_params=pltpu.CompilerParams(
            collective_id=0, has_side_effects=True, vmem_limit_bytes=58 * 2**20
        ),
    )(activations[0], norm_gain, expert_ids.reshape(1, tokens), in_proj[0], out_proj[0])
    return out[None]


def solution(mesh):
    return jax.shard_map(
        per_device,
        mesh=mesh,
        in_specs=(
            P("section", "expert", None),
            P("section", None),
            P("section", None, "expert"),
            P("section", "expert", None),
            P("section", "expert", None),
        ),
        out_specs=P("section", "expert", None),
        check_vma=False,
    )
```
